256 devices in a mesh: ens: 2 (over z_lo), ctx: 16 (over y, x), group: 8 (over z_hi, core).
Axes of the slice: x: 4, y: 4, z: 8 (z_hi: 4, z_lo: 2; z = z_hi * 2 + z_lo), core: 2. Of those that a mesh axis runs over, the one named last changes fastest.
Arguments:
- latents: bfloat16 [32, 4096, 512], P('ens', ('ctx', 'group')), parts along dimension 0, may hold values from -6 to 6
- rotary_rows: bfloat16 [32, 4096, 64], P('ens', ('ctx', 'group')), parts along dimension 0, may hold values from -6 to 6
- latent_gain: float32 [512], replicated, may hold values from 0.25 to 1.75
- key_up: bfloat16 [1024, 16, 128], P('ens', 'group'), parts along dimension 0, may hold values from -0.25 to 0.25
- value_up: bfloat16 [1024, 16, 128], P('ens', 'group'), parts along dimension 0, may hold values from -0.25 to 0.25
Outputs:
- stored_keys: bfloat16 [32, 16, 192, 4096], P(('ens', 'ctx'), 'group'), parts along dimension 0
- stored_values: bfloat16 [32, 4096, 16, 128], P(('ens', 'ctx'), None, 'group'), parts along dimension 0
The draws below stay inside these ranges and needn't reach their ends.
There are 2 independent parts, one for each index of `ens`. The reference program is written for one: setup_inputs(seed, part) draws one part's arguments, and reference() takes and returns one part's arrays. A program takes and returns all parts, laid end to end along the dimension named above; an argument that names none is the same for every part. Nothing has to cross between parts.
All inputs are finite; a program needn't handle non-finite values.
Results may differ from the reference program's by a relative error of at most 0.0049.
Values may be sent and summed in bfloat16 or wider, within the bound.
A program may use at most 64 MiB of HBM per device.

```python
import jax
import jax.numpy as jnp
from jax import lax

BATCH = 16
LENGTH = 4096
HEADS = 16
LATENT = 512
KEY_PART = 128
ROTARY = 64
VALUE_SIZE = 128


def levels(key, extent, split, low, top_value):
    loudness, own = 1.0, jax.random.fold_in(key, 6)
    for axis_at, shards_of in split:
        steps = jnp.exp(jax.random.uniform(jax.random.fold_in(own, axis_at), (shards_of,), jnp.float32, low / len(split), top_value / len(split)))
        loudness = loudness * jnp.repeat(steps, extent[axis_at] // shards_of).reshape([-1 if axis == axis_at else 1 for axis in range(len(extent))])
    return loudness


def gaussian(own_key, dims, width, reach, split=(), dtype=jnp.bfloat16):
    array = jax.random.normal(own_key, dims, jnp.float32) * width
    if len(split) > 0:
        array = levels(own_key, dims, split, -0.22, 0.18) * array
    return jnp.clip(array, min=-reach, max=reach).astype(dtype)


def setup_inputs(seed: int = 0, part: int = 0) -> dict:
    arg_keys = jax.random.split(jax.random.key(seed), 6)
    own_keys = jax.random.split(jax.random.fold_in(arg_keys[5], part), 6)
    latents = gaussian(own_keys[0], (BATCH, LENGTH, LATENT), 1.0, 6.0, ((1, 128),))
    rotary_rows = gaussian(own_keys[1], (BATCH, LENGTH, ROTARY), 1.0, 6.0, ((1, 128),))
    latent_gain = jnp.clip(1.0 + 0.15 * jax.random.normal(arg_keys[2], (LATENT,), jnp.float32), 0.25, 1.75)
    key_up = gaussian(own_keys[3], (LATENT, HEADS, KEY_PART), LATENT ** -0.5, 0.25, ((1, 8),))
    value_up = gaussian(own_keys[4], (LATENT, HEADS, VALUE_SIZE), LATENT ** -0.5, 0.25, ((1, 8),))
    return dict(latents=latents, rotary_rows=rotary_rows, latent_gain=latent_gain, key_up=key_up, value_up=value_up)


def root_norm(vectors, row_gain):
    return vectors * lax.rsqrt(lax.optimization_barrier(jnp.mean(vectors * vectors, axis=-1, keepdims=True)) + 1e-06) * row_gain

def reference(latents, rotary_rows, latent_gain, key_up, value_up):
    rows_ready = root_norm(latents.astype(jnp.float32), latent_gain).astype(jnp.bfloat16)
    rows_ready = lax.optimization_barrier(rows_ready)

    def expand_one(one):
        rows_one, rotary_one = one
        wide_keys = jnp.einsum('tr,rhk->thk', rows_one.astype(jnp.float32), key_up.astype(jnp.float32)).astype(jnp.bfloat16)
        shared = jnp.broadcast_to(rotary_one[:, None], (LENGTH, HEADS, ROTARY))
        wide_values = jnp.einsum('tr,rhk->thk', rows_one.astype(jnp.float32), value_up.astype(jnp.float32)).astype(jnp.bfloat16)
        return (jnp.concatenate([wide_keys, shared], axis=-1), wide_values)
    stored_keys, stored_values = lax.map(expand_one, (rows_ready, rotary_rows))
    stored_keys = jnp.transpose(stored_keys, (0, 2, 3, 1))
    return (stored_keys, stored_values)
```

```python
import jax
import jax.numpy as jnp
from jax import lax
from jax.experimental import pallas as pl
from jax.experimental.pallas import tpu as pltpu
from jax.sharding import PartitionSpec as P

MESH = pl.DeviceIdType.MESH
F32 = jnp.float32
BF16 = jnp.bfloat16
LAG_B, LAG_C, LAG_D = 3, 7, 8
ROT_SEND, ROT_PASS, ROT_PAIR, ROT_DONE = 6, 9, 13, 15


def gray(i):
    return i + i // 2 - 2 * (i // 3)


def kernel(lat, rot, gain, kup, vup, keys_out, vals_out,
           latv, rows, stage, rotv, rxb, ryb, rrows, kraw, vraw, gainv, wtmp, kt, vw, vtmp,
           loc_sem, xs_send, xs_recv, xy_recv, y_send,
           z1_send, z1_recv, z2_send, z2_recv, d_send, d_recv,
           rx_send, rx_recv, ry_send, ry_recv,
           rz_send, rz_recv, rd_send, rd_recv):
    e, c, g = lax.axis_index("ens"), lax.axis_index("ctx"), lax.axis_index("group")
    x, y = c % 4, c // 4
    partner = g + 1 - 2 * (g % 2)

    def at_xy(xx, yy):
        return (e, yy * 4 + xx, g)

    def at_group(gg):
        return (e, c, gg)

    def remote(src, dst, send, recv, dev):
        return pltpu.make_async_remote_copy(
            src_ref=src, dst_ref=dst, send_sem=send, recv_sem=recv,
            device_id=dev, device_id_type=MESH)

    barrier = pltpu.get_barrier_semaphore()
    for i in range(1, 4):
        pl.semaphore_signal(barrier, inc=1, device_id=at_xy((x + i) % 4, y), device_id_type=MESH)
        pl.semaphore_signal(barrier, inc=1, device_id=at_xy(x, (y + i) % 4), device_id_type=MESH)
    for gg in ((g + 2) % 8, (g + 6) % 8, partner):
        pl.semaphore_signal(barrier, inc=1, device_id=at_group(gg), device_id_type=MESH)

    local = [
        pltpu.make_async_copy(lat.at[c], rows.at[c, g], loc_sem.at[0]),
        pltpu.make_async_copy(lat, latv, loc_sem.at[1]),
        pltpu.make_async_copy(rot, rotv, loc_sem.at[2]),
        pltpu.make_async_copy(kup, kraw, loc_sem.at[3]),
        pltpu.make_async_copy(vup, vraw, loc_sem.at[4]),
        pltpu.make_async_copy(gain, gainv, loc_sem.at[5]),
    ]
    for copy in local:
        copy.start()
    local[0].wait()
    local[1].wait()
    pl.semaphore_wait(barrier, 9)

    def column_of(t):
        return ((y + gray(t // 4)) % 4) * 4 + (x + gray(t % 4)) % 4

    def z1(t, way):
        k = column_of(t)
        block = rows.at[k, g]
        return remote(block, block, z1_send.at[way, t], z1_recv.at[way, t],
                      at_group((g + 2 + 4 * way) % 8))

    def z1_wait(t, way):
        k = column_of(t)
        block = rows.at[k, (g + 6 + 4 * way) % 8]
        remote(block, block, z1_send.at[way, t], z1_recv.at[way, t], at_group(g)).wait_recv()

    def z2(t):
        k = column_of(t)
        way = t % 2
        block = rows.at[k, (g + 6 + 4 * way) % 8]
        return remote(block, block, z2_send.at[t], z2_recv.at[t],
                      at_group((g + 2 + 4 * way) % 8))

    def z2_wait(t):
        k = column_of(t)
        block = rows.at[k, (g + 4) % 8]
        remote(block, block, z2_send.at[t], z2_recv.at[t], at_group(g)).wait_recv()

    def push(t, hop):
        block = rows.at[column_of(t), (g + 2 * hop) % 8]
        return remote(block, block, d_send.at[hop, t], d_recv.at[hop, t], at_group(partner))

    def pushed(t, hop):
        block = rows.at[column_of(t), (partner + 2 * hop) % 8]
        remote(block, block, d_send.at[hop, t], d_recv.at[hop, t], at_group(g)).wait_recv()

    def x_direct(i):
        to = (x + 4 - gray(i)) % 4
        return remote(latv.at[y * 4 + to], rows.at[c, g], xs_send.at[i, 0], xy_recv.at[i],
                      at_xy(to, y))

    def x_stage(i, j):
        to = (x + 4 - gray(i)) % 4
        last = (y + 4 - gray(j)) % 4
        return remote(latv.at[last * 4 + to], stage.at[j - 1, i], xs_send.at[i, j],
                      xs_recv.at[i, j], at_xy(to, y))

    def y_send_of(i, j):
        to = (y + 4 - gray(j)) % 4
        if i == 0:
            src = latv.at[to * 4 + x]
        else:
            src = stage.at[j - 1, i]
        return remote(src, rows.at[y * 4 + (x + gray(i)) % 4, g], y_send.at[i, j],
                      xy_recv.at[4 * j + i], at_xy(x, to))

    def arrived(t):
        block = rows.at[column_of(t), g]
        remote(block, block, y_send.at[0, 0], xy_recv.at[t], at_xy(x, y)).wait_recv()

    def rx(i):
        to = (x + 4 - gray(i)) % 4
        return remote(rotv.at[:, to], rxb.at[x], rx_send.at[i], rx_recv.at[i], at_xy(to, y))

    def rx_wait(i):
        remote(rxb.at[0], rxb.at[(x + gray(i)) % 4], rx_send.at[i], rx_recv.at[i],
               at_xy(x, y)).wait_recv()

    def ry(j):
        to = (y + 4 - gray(j)) % 4
        return remote(rxb.at[:, to], ryb.at[y], ry_send.at[j], ry_recv.at[j], at_xy(x, to))

    def ry_wait(j):
        remote(ryb.at[0], ryb.at[(y + gray(j)) % 4], ry_send.at[j], ry_recv.at[j],
               at_xy(x, y)).wait_recv()

    def rz1(way):
        return remote(rrows.at[g], rrows.at[g], rz_send.at[way], rz_recv.at[way],
                      at_group((g + 2 + 4 * way) % 8))

    def rz1_wait(way):
        block = rrows.at[(g + 6 + 4 * way) % 8]
        remote(block, block, rz_send.at[way], rz_recv.at[way], at_group(g)).wait_recv()

    def rz2(way):
        block = rrows.at[(g + 6 + 4 * way) % 8, pl.ds(4 * way, 4)]
        return remote(block, block, rz_send.at[2 + way], rz_recv.at[2 + way],
                      at_group((g + 2 + 4 * way) % 8))

    def rz2_wait(way):
        block = rrows.at[(g + 4) % 8, pl.ds(4 * way, 4)]
        remote(block, block, rz_send.at[2 + way], rz_recv.at[2 + way], at_group(g)).wait_recv()

    def rpush(hop):
        block = rrows.at[(g + 2 * hop) % 8]
        return remote(block, block, rd_send.at[hop], rd_recv.at[hop], at_group(partner))

    def rpushed(hop):
        block = rrows.at[(partner + 2 * hop) % 8]
        remote(block, block, rd_send.at[hop], rd_recv.at[hop], at_group(g)).wait_recv()

    for way in range(2):
        z1(0, way).start()
    for i in range(1, 4):
        x_direct(i).start()
    for j in range(1, 4):
        y_send_of(0, j).start()
    for j in range(1, 4):
        for i in range(1, 4):
            x_stage(i, j).start()
    push(0, 0).start()
    local[2].wait()
    for i in range(1, 4):
        rx(i).start()
    rxb[pl.ds(x, 1)] = rotv[:, pl.ds(x, 1)].reshape(1, 4, 32, 64)

    @pl.loop(1, 16 + LAG_D)
    def _(t):
        @pl.when(t < 16)
        def _():
            arrived(t)
            for way in range(2):
                z1(t, way).start()
            push(t, 0).start()

        @pl.when(t == 3)
        def _():
            for j in range(1, 4):
                for i in range(1, 4):
                    block = stage.at[j - 1, i]
                    remote(block, block, xs_send.at[i, j], xs_recv.at[i, j],
                           at_xy(x, y)).wait_recv()
                    y_send_of(i, j).start()
            for i in range(1, 4):
                rx_wait(i)
            for j in range(1, 4):
                ry(j).start()
            ryb[pl.ds(y, 1)] = rxb[:, pl.ds(y, 1)].reshape(1, 4, 32, 64)

        @pl.when(t == 4)
        def _():
            for copy in local[3:]:
                copy.wait()
            wtmp[...] = kraw[...].astype(F32)
            for h in range(2):
                kt[pl.ds(h * 128, 128), :] = wtmp[pl.ds(h, 512, 2), :].T.astype(BF16)
            wtmp[...] = vraw[...].astype(F32)
            for h in range(2):
                vw[:, pl.ds(h * 128, 128)] = wtmp[pl.ds(h, 512, 2), :].astype(BF16)

        @pl.when(t == ROT_SEND - 1)
        def _():
            for j in range(1, 4):
                ry_wait(j)
            low, high = ryb[0:2], ryb[2:4]
            rrows[pl.ds(g, 1)] = jnp.concatenate([low, high], axis=-1).reshape(1, 8, 32, 128)

        @pl.when(t == ROT_SEND)
        def _():
            for way in range(2):
                rz1(way).start()
            rpush(0).start()

        @pl.when((t >= LAG_B) & (t < 16 + LAG_B))
        def _():
            u = t - LAG_B
            for way in range(2):
                z1_wait(u, way)
            z2(u).start()
            push(u, 3).start()
            push(u, 1).start()

        @pl.when(t == ROT_PASS)
        def _():
            for way in range(2):
                rz1_wait(way)
            for way in range(2):
                rz2(way).start()
            rpush(3).start()
            rpush(1).start()

        @pl.when(t == ROT_PAIR)
        def _():
            for way in range(2):
                rz2_wait(way)
            rpush(2).start()

        @pl.when((t >= LAG_C) & (t < 16 + LAG_C))
        def _():
            u = t - LAG_C
            z2_wait(u)
            push(u, 2).start()

        @pl.when(t >= LAG_D)
        def _():
            u = t - LAG_D
            for hop in range(4):
                pushed(u, hop)
            k = column_of(u)
            one = rows[pl.ds(k, 1)].reshape(256, 512).astype(F32)
            mean = jnp.mean(one * one, axis=-1, keepdims=True)
            ready = (one * lax.rsqrt(mean + 1e-06) * gainv[...]).astype(BF16)
            wide = lax.dot_general(kt[...], ready, (((1,), (1,)), ((), ())),
                                   preferred_element_type=F32)
            at = pl.ds(pl.multiple_of(k * 256, 256), 256)
            for h in range(2):
                keys_out[h, pl.ds(0, 128), at] = wide[h * 128:(h + 1) * 128].astype(BF16)
            vals = jnp.dot(ready, vw[...], preferred_element_type=F32)
            for h in range(2):
                vtmp[pl.ds(h, 256, 2), :] = vals[:, h * 128:(h + 1) * 128]
            vals_out[pl.ds(pl.multiple_of(k * 512, 512), 512), :] = vtmp[...].astype(BF16)

        @pl.when(t == ROT_DONE)
        def _():
            for hop in range(4):
                rpushed(hop)

            @pl.loop(0, 8)
            def _(n):
                pair = rrows[:, pl.ds(n, 1)].reshape(256, 128).astype(F32).T.astype(BF16)
                for half in range(2):
                    at = pl.ds(pl.multiple_of((n + 8 * half) * 256, 256), 256)
                    for h in range(2):
                        keys_out[h, pl.ds(128, 64), at] = pair[half * 64:(half + 1) * 64]

    for i in range(1, 4):
        for j in range(4):
            block = stage.at[0, 0]
            remote(block, block, xs_send.at[i, j], xy_recv.at[0], at_xy(x, y)).wait_send()
    for i in range(4):
        for j in range(1, 4):
            block = stage.at[0, 0]
            remote(block, block, y_send.at[i, j], xy_recv.at[0], at_xy(x, y)).wait_send()
    for i in range(1, 4):
        rx(i).wait_send()
        ry(i).wait_send()
    for way in range(2):
        rz1(way).wait_send()
        rz2(way).wait_send()
    for hop in range(4):
        rpush(hop).wait_send()

    @pl.loop(0, 16)
    def _(t):
        for way in range(2):
            z1(t, way).wait_send()
        z2(t).wait_send()
        for hop in range(4):
            push(t, hop).wait_send()


def per_device(latents, rotary_rows, latent_gain, key_up, value_up):
    dma = pltpu.SemaphoreType.DMA
    any_spec = pl.BlockSpec(memory_space=pltpu.HBM)
    keys, vals = pl.pallas_call(
        kernel,
        out_shape=(
            jax.ShapeDtypeStruct((2, 192, 4096), BF16),
            jax.ShapeDtypeStruct((8192, 128), BF16),
        ),
        in_specs=[any_spec] * 5,
        out_specs=[pl.BlockSpec(memory_space=pltpu.VMEM)] * 2,
        scratch_shapes=[
            pltpu.VMEM((16, 32, 512), BF16),
            pltpu.VMEM((16, 8, 32, 512), BF16),
            pltpu.VMEM((3, 4, 32, 512), BF16),
            pltpu.VMEM((4, 4, 32, 64), BF16),
            pltpu.VMEM((4, 4, 32, 64), BF16),
            pltpu.VMEM((4, 4, 32, 64), BF16),
            pltpu.VMEM((8, 8, 32, 128), BF16),
            pltpu.VMEM((1024, 128), BF16),
            pltpu.VMEM((1024, 128), BF16),
            pltpu.VMEM((1, 512), F32),
            pltpu.VMEM((1024, 128), F32),
            pltpu.VMEM((256, 512), BF16),
            pltpu.VMEM((512, 256), BF16),
            pltpu.VMEM((512, 128), F32),
            dma((7,)),
            dma((4, 4)), dma((4, 4)), dma((16,)), dma((4, 4)),
            dma((2, 16)), dma((2, 16)), dma((16,)), dma((16,)), dma((4, 16)), dma((4, 16)),
            dma((4,)), dma((4,)), dma((4,)), dma((4,)),
            dma((4,)), dma((4,)), dma((4,)), dma((4,)),
        ],
        compiler_params=pltpu.CompilerParams(
            collective_id=0, has_side_effects=True, vmem_limit_bytes=40 * 1024 * 1024),
        name="expand",
    )(*(pltpu.with_memory_space_constraint(a, pltpu.HBM) for a in (
        latents, rotary_rows.reshape(4, 4, 32, 64), latent_gain.reshape(1, 512),
        key_up.reshape(1024, 128), value_up.reshape(1024, 128))))
    return keys.reshape(1, 2, 192, 4096), vals.reshape(1, 4096, 2, 128)


def solution(mesh):
    in_specs = (
        P("ens", ("ctx", "group"), None),
        P("ens", ("ctx", "group"), None),
        P(),
        P("ens", "group", None),
        P("ens", "group", None),
    )
    out_specs = (P(("ens", "ctx"), "group", None, None), P(("ens", "ctx"), None, "group", None))
    return jax.shard_map(
        per_device, mesh=mesh, in_specs=in_specs, out_specs=out_specs, check_vma=False
    )
```

```python
import jax
import jax.numpy as jnp
from jax import lax
from jax.experimental import pallas as pl
from jax.experimental.pallas import tpu as pltpu
from jax.sharding import PartitionSpec as P

MESH = pl.DeviceIdType.MESH
F32 = jnp.float32
BF16 = jnp.bfloat16
LAG_B, LAG_C, LAG_D = 3, 7, 8
ROT_Z, ROT_X, ROT_Y, ROT_PUSH, ROT_DONE = 4, 8, 11, 14, 16


def gray(i):
    return i + i // 2 - 2 * (i // 3)


def kernel(lat, rot, gain, kup, vup, keys_out, vals_out,
           latv, rows, stage, rotv, rz, rx, ry, rt, kraw, vraw, gainv, wtmp, kt, vw, vtmp,
           loc_sem, x_send, y_send, z_send, d_send, r_send,
           xs_recv, xy_recv, z1_recv, z2_recv, d_recv,
           rz1_recv, rz2_recv, rx_recv, ry_recv, rd_recv):
    e, c, g = lax.axis_index("ens"), lax.axis_index("ctx"), lax.axis_index("group")
    x, y = c % 4, c // 4
    zh, core = g // 2, g % 2
    partner = g + 1 - 2 * core

    def at_xy(xx, yy):
        return (e, yy * 4 + xx, g)

    def at_group(gg):
        return (e, c, gg)

    def remote(src, dst, send, recv, dev):
        return pltpu.make_async_remote_copy(
            src_ref=src, dst_ref=dst, send_sem=send, recv_sem=recv,
            device_id=dev, device_id_type=MESH)

    def got(block, recv):
        remote(block, block, x_send, recv, at_group(g)).wait_recv()

    def sent(block, send):
        remote(block, block, send, xy_recv.at[0], at_group(g)).wait_send()

    barrier = pltpu.get_barrier_semaphore()
    for i in range(1, 4):
        pl.semaphore_signal(barrier, inc=1, device_id=at_xy((x + i) % 4, y), device_id_type=MESH)
        pl.semaphore_signal(barrier, inc=1, device_id=at_xy(x, (y + i) % 4), device_id_type=MESH)
    for gg in ((g + 2) % 8, (g + 6) % 8, partner):
        pl.semaphore_signal(barrier, inc=1, device_id=at_group(gg), device_id_type=MESH)

    local = [
        pltpu.make_async_copy(rot, rotv, loc_sem.at[0]),
        pltpu.make_async_copy(lat.at[c], rows.at[c, g], loc_sem.at[1]),
        pltpu.make_async_copy(lat, latv, loc_sem.at[2]),
        pltpu.make_async_copy(kup, kraw, loc_sem.at[3]),
        pltpu.make_async_copy(vup, vraw, loc_sem.at[4]),
        pltpu.make_async_copy(gain, gainv, loc_sem.at[5]),
    ]
    for copy in local:
        copy.start()
    local[0].wait()
    rz[pl.ds(zh, 1)] = jnp.concatenate([rotv[0:2], rotv[2:4]], axis=-1).reshape(1, 2, 4, 32, 128)
    local[1].wait()
    local[2].wait()
    pl.semaphore_wait(barrier, 9)

    def column_of(t):
        far, both = (t + 12) // 16, (t + 9) // 16
        i = (1 - far) * t + both * (1 + (t + 2) % 3)
        j = far * (1 - both) * (t - 3) + both * ((t + 2) // 3 - 2)
        return ((y + gray(j)) % 4) * 4 + (x + gray(i)) % 4

    def order(i, j):
        return i if j == 0 else 3 + j if i == 0 else 3 + 3 * j + i

    def along(way):
        return at_group((g + 2 + 4 * way) % 8)

    def z1(t, way):
        block = rows.at[column_of(t), g]
        return remote(block, block, z_send, z1_recv.at[t], along(way))

    def z2(t):
        way = t % 2
        block = rows.at[column_of(t), (g + 6 + 4 * way) % 8]
        return remote(block, block, z_send, z2_recv.at[t], along(way))

    def push(t, hop):
        block = rows.at[column_of(t), (g + 2 * hop) % 8]
        return remote(block, block, d_send, d_recv.at[t], at_group(partner))

    def x_direct(i):
        to = (x + 4 - gray(i)) % 4
        return remote(latv.at[y * 4 + to], rows.at[c, g], x_send, xy_recv.at[i], at_xy(to, y))

    def x_stage(i, j):
        to = (x + 4 - gray(i)) % 4
        last = (y + 4 - gray(j)) % 4
        return remote(latv.at[last * 4 + to], stage.at[j - 1, i - 1], x_send,
                      xs_recv.at[i, j], at_xy(to, y))

    def y_on(i, j):
        to = (y + 4 - gray(j)) % 4
        src = latv.at[to * 4 + x] if i == 0 else stage.at[j - 1, i - 1]
        return remote(src, rows.at[y * 4 + (x + gray(i)) % 4, g], y_send,
                      xy_recv.at[order(i, j)], at_xy(x, to))

    def rz1(way):
        return remote(rz.at[zh], rz.at[zh], r_send.at[0], rz1_recv.at[way], along(way))

    def rz2(way):
        block = rz.at[(zh + 3 + 2 * way) % 4, way]
        return remote(block, block, r_send.at[0], rz2_recv.at[way], along(way))

    def rx_to(i):
        to = (x + 4 - gray(i)) % 4
        return remote(rz.at[:, :, to], rx.at[x], r_send.at[1], rx_recv.at[i], at_xy(to, y))

    def ry_to(j):
        to = (y + 4 - gray(j)) % 4
        return remote(rx.at[:, :, to % 2], ry.at[y, :, :, core], r_send.at[2], ry_recv.at[j],
                      at_xy(x, to))

    def rpush(j):
        block = ry.at[(y + gray(j)) % 4, :, :, core]
        return remote(block, block, r_send.at[3], rd_recv.at[j], at_group(partner))

    for way in range(2):
        z1(0, way).start()
    for way in range(2):
        rz1(way).start()
    for i in range(1, 4):
        x_direct(i).start()
        y_on(0, i).start()
    push(0, 0).start()

    @pl.loop(1, 16 + LAG_D)
    def _(t):
        @pl.when(t < 16)
        def _():
            got(rows.at[column_of(t), g], xy_recv.at[t])
            for way in range(2):
                z1(t, way).start()
            push(t, 0).start()

        @pl.when(t == 2)
        def _():
            for j in range(1, 4):
                for i in range(1, 4):
                    x_stage(i, j).start()

        for j in range(1, 4):
            @pl.when(t == 3 + j)
            def _(j=j):
                for i in range(1, 4):
                    got(stage.at[j - 1, i - 1], xs_recv.at[i, j])
                    y_on(i, j).start()

        @pl.when(t == 7)
        def _():
            for copy in local[3:]:
                copy.wait()
            wtmp[...] = kraw[...].astype(F32)
            for h in range(2):
                kt[pl.ds(h * 128, 128), :] = wtmp[pl.ds(h, 512, 2), :].T.astype(BF16)
            wtmp[...] = vraw[...].astype(F32)
            for h in range(2):
                vw[:, pl.ds(h * 128, 128)] = wtmp[pl.ds(h, 512, 2), :].astype(BF16)

        @pl.when((t >= LAG_B) & (t < 16 + LAG_B))
        def _():
            u = t - LAG_B
            got(rows.at[column_of(u), pl.ds(0, 2)], z1_recv.at[u])
            z2(u).start()
            push(u, 3).start()
            push(u, 1).start()

        @pl.when(t == ROT_Z)
        def _():
            for way in range(2):
                got(rz.at[0], rz1_recv.at[way])
            for way in range(2):
                rz2(way).start()

        @pl.when(t == ROT_X)
        def _():
            for way in range(2):
                got(rz.at[0, 0], rz2_recv.at[way])
            for i in range(1, 4):
                rx_to(i).start()
            rx[pl.ds(x, 1)] = rz[:, :, pl.ds(x, 1)].reshape(1, 4, 2, 32, 128)

        @pl.when(t == ROT_Y)
        def _():
            for i in range(1, 4):
                got(rx.at[0], rx_recv.at[i])
            for j in range(1, 4):
                ry_to(j).start()
            ry[pl.ds(y, 1), :, :, pl.ds(core, 1)] = rx[:, :, pl.ds(y % 2, 1)].reshape(
                1, 4, 4, 1, 32, 128)

        @pl.when(t == ROT_PUSH)
        def _():
            rpush(0).start()
            for j in range(1, 4):
                got(ry.at[0, :, :, 0], ry_recv.at[j])
                rpush(j).start()

        @pl.when((t >= LAG_C) & (t < 16 + LAG_C))
        def _():
            u = t - LAG_C
            got(rows.at[column_of(u), 0], z2_recv.at[u])
            push(u, 2).start()

        @pl.when(t >= LAG_D)
        def _():
            u = t - LAG_D
            k = column_of(u)
            got(rows.at[k, pl.ds(0, 4)], d_recv.at[u])
            one = rows[pl.ds(k, 1)].reshape(256, 512).astype(F32)
            mean = jnp.mean(one * one, axis=-1, keepdims=True)
            ready = (one * lax.rsqrt(mean + 1e-06) * gainv[...]).astype(BF16)
            wide = lax.dot_general(kt[...], ready, (((1,), (1,)), ((), ())),
                                   preferred_element_type=F32)
            at = pl.ds(pl.multiple_of(k * 256, 256), 256)
            for h in range(2):
                keys_out[h, pl.ds(0, 128), at] = wide[h * 128:(h + 1) * 128].astype(BF16)
            vals = jnp.dot(ready, vw[...], preferred_element_type=F32)
            for h in range(2):
                vtmp[pl.ds(h, 256, 2), :] = vals[:, h * 128:(h + 1) * 128]
            vals_out[pl.ds(pl.multiple_of(k * 512, 512), 512), :] = vtmp[...].astype(BF16)

        @pl.when(t == ROT_DONE)
        def _():
            for j in range(4):
                got(ry.at[0, :, :, 0], rd_recv.at[j])

            @pl.loop(0, 16)
            def _(k):
                one = ry[pl.ds(k // 4, 1), pl.ds(k % 4, 1)].reshape(256, 128)
                rt[...] = one.astype(F32).T
                half = rt[pl.ds(pl.multiple_of(y // 2 * 64, 64), 64), :].astype(BF16)
                at = pl.ds(pl.multiple_of(k * 256, 256), 256)
                for h in range(2):
                    keys_out[h, pl.ds(128, 64), at] = half

    sent(latv.at[pl.ds(0, 12)], x_send)
    sent(latv.at[pl.ds(0, 12)], y_send)
    sent(rows.at[pl.ds(0, 6)], z_send)
    sent(rows.at[pl.ds(0, 8)], d_send)
    sent(rz.at[pl.ds(0, 3)], r_send.at[0])
    sent(rx.at[pl.ds(0, 3)], r_send.at[1])
    sent(ry.at[pl.ds(0, 3), :, :, 0], r_send.at[2])
    sent(ry.at[:, :, :, 0], r_send.at[3])


def per_device(latents, rotary_rows, latent_gain, key_up, value_up):
    dma = pltpu.SemaphoreType.DMA
    in_hbm = pl.BlockSpec(memory_space=pltpu.HBM)
    keys, vals = pl.pallas_call(
        kernel,
        out_shape=(
            jax.ShapeDtypeStruct((2, 192, 4096), BF16),
            jax.ShapeDtypeStruct((8192, 128), BF16),
        ),
        in_specs=[in_hbm] * 5,
        out_specs=[pl.BlockSpec(memory_space=pltpu.VMEM)] * 2,
        scratch_shapes=[
            pltpu.VMEM((16, 32, 512), BF16),
            pltpu.VMEM((16, 8, 32, 512), BF16),
            pltpu.VMEM((3, 3, 32, 512), BF16),
            pltpu.VMEM((4, 4, 32, 64), BF16),
            pltpu.VMEM((4, 2, 4, 32, 128), BF16),
            pltpu.VMEM((4, 4, 2, 32, 128), BF16),
            pltpu.VMEM((4, 4, 4, 2, 32, 128), BF16),
            pltpu.VMEM((128, 256), F32),
            pltpu.VMEM((1024, 128), BF16),
            pltpu.VMEM((1024, 128), BF16),
            pltpu.VMEM((1, 512), F32),
            pltpu.VMEM((1024, 128), F32),
            pltpu.VMEM((256, 512), BF16),
            pltpu.VMEM((512, 256), BF16),
            pltpu.VMEM((512, 128), F32),
            dma((6,)), dma, dma, dma, dma, dma((4,)),
            dma((4, 4)), dma((16,)), dma((16,)), dma((16,)), dma((16,)),
            dma((2,)), dma((2,)), dma((4,)), dma((4,)), dma((4,)),
        ],
        compiler_params=pltpu.CompilerParams(
            collective_id=0, has_side_effects=True, vmem_limit_bytes=40 * 1024 * 1024),
        name="expand",
    )(*(pltpu.with_memory_space_constraint(a, pltpu.HBM) for a in (
        latents, rotary_rows.reshape(4, 4, 32, 64), latent_gain.reshape(1, 512),
        key_up.reshape(1024, 128), value_up.reshape(1024, 128))))
    return keys.reshape(1, 2, 192, 4096), vals.reshape(1, 4096, 2, 128)


def solution(mesh):
    in_specs = (
        P("ens", ("ctx", "group"), None),
        P("ens", ("ctx", "group"), None),
        P(),
        P("ens", "group", None),
        P("ens", "group", None),
    )
    out_specs = (P(("ens", "ctx"), "group", None, None), P(("ens", "ctx"), None, "group", None))
    return jax.shard_map(
        per_device, mesh=mesh, in_specs=in_specs, out_specs=out_specs, check_vma=False
    )
```

```python
import jax
import jax.numpy as jnp
from jax import lax
from jax.experimental import pallas as pl
from jax.experimental.pallas import tpu as pltpu
from jax.sharding import PartitionSpec as P

MESH = pl.DeviceIdType.MESH
F32 = jnp.float32
BF16 = jnp.bfloat16
LAG_B, LAG_C, LAG_D = 3, 7, 8
ROT_EACH = 4
LAST = 1
ROT_Z, ROT_X, ROT_Y, ROT_PUSH, ROT_DONE = 4, 8, 11, 14, 16


def gray(i):
    return i + i // 2 - 2 * (i // 3)


def column_of(t, x, y):
    far, both = (t + 12) // 16, (t + 9) // 16
    i = (1 - far) * t + both * (1 + (t + 2) % 3)
    j = far * (1 - both) * (t - 3) + both * ((t + 2) // 3 - 2)
    return ((y + gray(j)) % 4) * 4 + (x + gray(i)) % 4


def order(i, j):
    return i if j == 0 else 3 + j if i == 0 else 3 + 3 * j + i


def expand_chunk(k, put, rows, gainv, kt, vw, keys_out, vals_out, vtmp):
    one = rows[pl.ds(k, 1)].reshape(256, 512).astype(F32)
    mean = jnp.mean(one * one, axis=-1, keepdims=True)
    ready = (one * lax.rsqrt(mean + 1e-06) * gainv[...]).astype(BF16)
    wide = lax.dot_general(kt[...], ready, (((1,), (1,)), ((), ())),
                           preferred_element_type=F32)
    at = pl.ds(pl.multiple_of(put * 256, 256), 256)
    for h in range(2):
        keys_out[h, pl.ds(0, 128), at] = wide[h * 128:(h + 1) * 128].astype(BF16)
    vals = jnp.dot(ready, vw[...], preferred_element_type=F32)
    for h in range(2):
        vtmp[pl.ds(h, 256, 2), :] = vals[:, h * 128:(h + 1) * 128]
    vals_out[pl.ds(pl.multiple_of(put * 512, 512), 512), :] = vtmp[...].astype(BF16)


def kernel(lat, rot, gain, kup, vup, keys_out, vals_out, rows, gainv, kt, vw,
           latv, stage, rotv, rz, rx, ry, rt, kraw, vraw, wtmp, vtmp,
           loc_sem, send, d_send, xs_recv, xy_recv, z1_recv, z2_recv, d_recv, r_recv):
    e, c, g = lax.axis_index("ens"), lax.axis_index("ctx"), lax.axis_index("group")
    x, y = c % 4, c // 4
    zh, core = g // 2, g % 2
    partner = g + 1 - 2 * core

    def at_xy(xx, yy):
        return (e, yy * 4 + xx, g)

    def at_group(gg):
        return (e, c, gg)

    def remote(src, dst, send, recv, dev):
        return pltpu.make_async_remote_copy(
            src_ref=src, dst_ref=dst, send_sem=send, recv_sem=recv,
            device_id=dev, device_id_type=MESH)

    def got(block, recv):
        remote(block, block, send, recv, at_group(g)).wait_recv()

    def sent(block, sem):
        remote(block, block, sem, xy_recv.at[0], at_group(g)).wait_send()

    barrier = pltpu.get_barrier_semaphore()
    for i in range(1, 4):
        pl.semaphore_signal(barrier, inc=1, device_id=at_xy((x + i) % 4, y), device_id_type=MESH)
        pl.semaphore_signal(barrier, inc=1, device_id=at_xy(x, (y + i) % 4), device_id_type=MESH)
    for gg in ((g + 2) % 8, (g + 6) % 8, partner):
        pl.semaphore_signal(barrier, inc=1, device_id=at_group(gg), device_id_type=MESH)

    local = [
        pltpu.make_async_copy(rot, rotv, loc_sem.at[0]),
        pltpu.make_async_copy(lat.at[c], rows.at[c, g], loc_sem.at[1]),
        pltpu.make_async_copy(lat, latv, loc_sem.at[2]),
        pltpu.make_async_copy(kup, kraw, loc_sem.at[3]),
        pltpu.make_async_copy(vup, vraw, loc_sem.at[4]),
        pltpu.make_async_copy(gain, gainv, loc_sem.at[5]),
    ]
    for copy in local:
        copy.start()
    local[0].wait()
    rz[pl.ds(zh, 1)] = jnp.concatenate([rotv[0:2], rotv[2:4]], axis=-1).reshape(1, 2, 4, 32, 128)
    local[1].wait()
    local[2].wait()
    pl.semaphore_wait(barrier, 9)

    def along(way):
        return at_group((g + 2 + 4 * way) % 8)

    def z1(t, way):
        block = rows.at[column_of(t, x, y), g]
        return remote(block, block, send, z1_recv.at[t % 8], along(way))

    def z2(t):
        way = t % 2
        block = rows.at[column_of(t, x, y), (g + 6 + 4 * way) % 8]
        return remote(block, block, send, z2_recv.at[t % 8], along(way))

    def push(t, hop):
        block = rows.at[column_of(t, x, y), (g + 2 * hop) % 8]
        return remote(block, block, d_send, d_recv.at[t], at_group(partner))

    def x_direct(i):
        to = (x + 4 - gray(i)) % 4
        return remote(latv.at[y * 4 + to], rows.at[c, g], send, xy_recv.at[i], at_xy(to, y))

    def x_stage(i, j):
        to = (x + 4 - gray(i)) % 4
        last = (y + 4 - gray(j)) % 4
        return remote(latv.at[last * 4 + to], stage.at[j - 1, i - 1], send,
                      xs_recv.at[j - 1], at_xy(to, y))

    def y_on(i, j):
        to = (y + 4 - gray(j)) % 4
        src = latv.at[to * 4 + x] if i == 0 else stage.at[j - 1, i - 1]
        return remote(src, rows.at[y * 4 + (x + gray(i)) % 4, g], send,
                      xy_recv.at[order(i, j) if i * j == 0 else 6 + j], at_xy(x, to))

    def rz1(way):
        return remote(rz.at[zh], rz.at[zh], send, r_recv.at[0], along(way))

    def rz2(way):
        block = rz.at[(zh + 3 + 2 * way) % 4, way]
        return remote(block, block, send, r_recv.at[1], along(way))

    def rx_to(i):
        to = (x + 4 - gray(i)) % 4
        return remote(rz.at[:, :, to], rx.at[x], send, r_recv.at[2], at_xy(to, y))

    def ry_to(j):
        to = (y + 4 - gray(j)) % 4
        return remote(rx.at[:, :, to % 2], ry.at[y, :, :, core], send, r_recv.at[3],
                      at_xy(x, to))

    def rpush(j):
        block = ry.at[(y + gray(j)) % 4, :, :, core]
        return remote(block, block, send, r_recv.at[4], at_group(partner))

    for way in range(2):
        z1(0, way).start()
    for way in range(2):
        rz1(way).start()
    for i in range(1, 4):
        x_direct(i).start()
        y_on(0, i).start()
    push(0, 0).start()

    @pl.loop(1, 16 + LAG_D)
    def _(t):
        @pl.when(t < 16)
        def _():
            @pl.when(t < 7)
            def _():
                got(rows.at[column_of(t, x, y), g], xy_recv.at[t])

            for j in range(1, 4):
                @pl.when(t == 4 + 3 * j)
                def _(j=j):
                    got(latv.at[pl.ds(0, 3)], xy_recv.at[6 + j])

            for way in range(2):
                z1(t, way).start()
            push(t, 0).start()

        @pl.when(t == 2)
        def _():
            for j in range(1, 4):
                for i in range(1, 4):
                    x_stage(i, j).start()

        for j in range(1, 4):
            @pl.when(t == 3 + j)
            def _(j=j):
                got(stage.at[j - 1], xs_recv.at[j - 1])
                for i in range(1, 4):
                    y_on(i, j).start()

        @pl.when(t == 7)
        def _():
            for copy in local[3:]:
                copy.wait()
            wtmp[...] = kraw[...].astype(F32)
            for h in range(2):
                kt[pl.ds(h * 128, 128), :] = wtmp[pl.ds(h, 512, 2), :].T.astype(BF16)
            wtmp[...] = vraw[...].astype(F32)
            for h in range(2):
                vw[:, pl.ds(h * 128, 128)] = wtmp[pl.ds(h, 512, 2), :].astype(BF16)

        @pl.when((t >= LAG_B) & (t < 16 + LAG_B))
        def _():
            u = t - LAG_B
            got(rows.at[column_of(u, x, y), pl.ds(0, 2)], z1_recv.at[u % 8])
            z2(u).start()
            push(u, 3).start()
            push(u, 1).start()

        @pl.when(t == ROT_Z)
        def _():
            got(rz.at[pl.ds(0, 2)], r_recv.at[0])
            for way in range(2):
                rz2(way).start()

        @pl.when(t == ROT_X)
        def _():
            got(rz.at[0], r_recv.at[1])
            for i in range(1, 4):
                rx_to(i).start()
            rx[pl.ds(x, 1)] = rz[:, :, pl.ds(x, 1)].reshape(1, 4, 2, 32, 128)

        @pl.when(t == ROT_Y)
        def _():
            got(rx.at[pl.ds(0, 3)], r_recv.at[2])
            for j in range(1, 4):
                ry_to(j).start()
            ry[pl.ds(y, 1), :, :, pl.ds(core, 1)] = rx[:, :, pl.ds(y % 2, 1)].reshape(
                1, 4, 4, 1, 32, 128)

        @pl.when(t == ROT_PUSH)
        def _():
            got(ry.at[pl.ds(0, 3), :, :, 0], r_recv.at[3])
            for j in range(4):
                rpush(j).start()

        @pl.when((t >= LAG_C) & (t < 16 + LAG_C))
        def _():
            u = t - LAG_C
            got(rows.at[column_of(u, x, y), 0], z2_recv.at[u % 8])
            push(u, 2).start()

        @pl.when(t >= LAG_D)
        def _():
            u = t - LAG_D
            k = column_of(u, x, y)
            got(rows.at[k, pl.ds(0, 4)], d_recv.at[u])

            @pl.when(u < 16 - LAST)
            def _():
                expand_chunk(k, k, rows, gainv, kt, vw, keys_out, vals_out, vtmp)

        @pl.when(t == ROT_DONE)
        def _():
            got(ry.at[:, :, :, 0], r_recv.at[4])

        @pl.when((t >= ROT_DONE) & (t < ROT_DONE + 16 // ROT_EACH))
        def _():
            @pl.loop(0, ROT_EACH)
            def _(n):
                k = (t - ROT_DONE) * ROT_EACH + n
                one = ry[pl.ds(k // 4, 1), pl.ds(k % 4, 1)].reshape(256, 128)
                rt[...] = one.astype(F32).T
                half = rt[pl.ds(pl.multiple_of(y // 2 * 64, 64), 64), :].astype(BF16)
                at = pl.ds(pl.multiple_of(k * 256, 256), 256)
                for h in range(2):
                    keys_out[h, pl.ds(128, 64), at] = half

    sent(rows.at[pl.ds(0, 14)], send)
    sent(rows.at[pl.ds(0, 8)], d_send)


def store(keys_in, vals_in, rows, gainv, kt, vw, keys_out, vals_out, keys_last, vals_last, vtmp,
          keys_sem, vals_sem):
    c = lax.axis_index("ctx")
    x, y = c % 4, c // 4

    def put(k):
        return pl.ds(pl.multiple_of(k * 256, 256), 256), pl.ds(pl.multiple_of(k * 512, 512), 512)

    @pl.loop(0, 16 - LAST)
    def _(t):
        at, to = put(column_of(t, x, y))
        pltpu.make_async_copy(keys_in.at[:, :, at], keys_out.at[:, :, at], keys_sem).start()
        pltpu.make_async_copy(vals_in.at[to], vals_out.at[to], vals_sem).start()

    for n in range(LAST):
        at, to = put(column_of(16 - LAST + n, x, y))
        turned = pl.ds(128, 64)
        pltpu.make_async_copy(keys_in.at[:, turned, at], keys_out.at[:, turned, at],
                              keys_sem).start()

    @pl.loop(0, LAST)
    def _(n):
        k = column_of(16 - LAST + n, x, y)
        expand_chunk(k, n, rows, gainv, kt, vw, keys_last, vals_last, vtmp)

    for n in range(LAST):
        at, to = put(column_of(16 - LAST + n, x, y))
        here, there = put(n)
        pltpu.make_async_copy(keys_last.at[:, :, here], keys_out.at[:, pl.ds(0, 128), at],
                              keys_sem).start()
        pltpu.make_async_copy(vals_last.at[there], vals_out.at[to], vals_sem).start()
    pltpu.make_async_copy(keys_in, keys_out, keys_sem).wait()
    pltpu.make_async_copy(vals_in, vals_out, vals_sem).wait()


def per_device(latents, rotary_rows, latent_gain, key_up, value_up):
    dma = pltpu.SemaphoreType.DMA
    hbm = pl.BlockSpec(memory_space=pltpu.HBM)
    vmem = pl.BlockSpec(memory_space=pltpu.VMEM)
    outs = (
        jax.ShapeDtypeStruct((2, 192, 4096), BF16),
        jax.ShapeDtypeStruct((8192, 128), BF16),
    )
    parts = pl.pallas_call(
        kernel,
        out_shape=outs + (
            jax.ShapeDtypeStruct((16, 8, 32, 512), BF16),
            jax.ShapeDtypeStruct((1, 512), F32),
            jax.ShapeDtypeStruct((256, 512), BF16),
            jax.ShapeDtypeStruct((512, 256), BF16),
        ),
        in_specs=[hbm] * 5,
        out_specs=[vmem] * 6,
        scratch_shapes=[
            pltpu.VMEM((16, 32, 512), BF16),
            pltpu.VMEM((3, 3, 32, 512), BF16),
            pltpu.VMEM((4, 4, 32, 64), BF16),
            pltpu.VMEM((4, 2, 4, 32, 128), BF16),
            pltpu.VMEM((4, 4, 2, 32, 128), BF16),
            pltpu.VMEM((4, 4, 4, 2, 32, 128), BF16),
            pltpu.VMEM((128, 256), F32),
            pltpu.VMEM((1024, 128), BF16),
            pltpu.VMEM((1024, 128), BF16),
            pltpu.VMEM((1024, 128), F32),
            pltpu.VMEM((512, 128), F32),
            dma((6,)), dma, dma, dma((3,)), dma((10,)), dma((8,)), dma((8,)), dma((16,)), dma((5,)),
        ],
        compiler_params=pltpu.CompilerParams(
            collective_id=0, has_side_effects=True, vmem_limit_bytes=32 * 1024 * 1024),
        name="expand",
    )(*(pltpu.with_memory_space_constraint(a, pltpu.HBM) for a in (
        latents, rotary_rows.reshape(4, 4, 32, 64), latent_gain.reshape(1, 512),
        key_up.reshape(1024, 128), value_up.reshape(1024, 128))))
    keys, vals = pl.pallas_call(
        store,
        out_shape=outs,
        in_specs=[vmem] * 6,
        out_specs=[hbm] * 2,
        scratch_shapes=[
            pltpu.VMEM((2, 128, LAST * 256), BF16),
            pltpu.VMEM((LAST * 512, 128), BF16),
            pltpu.VMEM((512, 128), F32),
            dma, dma,
        ],
        compiler_params=pltpu.CompilerParams(vmem_limit_bytes=32 * 1024 * 1024),
        name="store",
    )(*parts)
    return keys.reshape(1, 2, 192, 4096), vals.reshape(1, 4096, 2, 128)


def solution(mesh):
    in_specs = (
        P("ens", ("ctx", "group"), None),
        P("ens", ("ctx", "group"), None),
        P(),
        P("ens", "group", None),
        P("ens", "group", None),
    )
    out_specs = (P(("ens", "ctx"), "group", None, None), P(("ens", "ctx"), None, "group", None))
    return jax.shard_map(
        per_device, mesh=mesh, in_specs=in_specs, out_specs=out_specs, check_vma=False
    )
```

```python
import jax
import jax.numpy as jnp
from jax import lax
from jax.experimental import pallas as pl
from jax.experimental.pallas import tpu as pltpu
from jax.sharding import PartitionSpec as P

MESH = pl.DeviceIdType.MESH
F32 = jnp.float32
BF16 = jnp.bfloat16
LAG_B, LAG_C, LAG_D = 3, 7, 8
LAST = 1
ROT_Z, ROT_X, ROT_Y, ROT_PUSH, ROT_DONE = 4, 8, 11, 15, 17


def gray(i):
    return i + i // 2 - 2 * (i // 3)


def column_of(t, x, y):
    far, both = (t + 12) // 16, (t + 9) // 16
    i = (1 - far) * t + both * (1 + (t + 2) % 3)
    j = far * (1 - both) * (t - 3) + both * ((t + 2) // 3 - 2)
    return ((y + gray(j)) % 4) * 4 + (x + gray(i)) % 4


def order(i, j):
    return i if j == 0 else 3 + j if i == 0 else 3 + 3 * j + i


def expand_chunk(k, put, rows, gainv, kt, vw, keys_out, vals_out, vtmp):
    one = rows[pl.ds(k, 1)].reshape(256, 512).astype(F32)
    mean = jnp.mean(one * one, axis=-1, keepdims=True)
    ready = (one * lax.rsqrt(mean + 1e-06) * gainv[...]).astype(BF16)
    wide = lax.dot_general(kt[...], ready, (((1,), (1,)), ((), ())),
                           preferred_element_type=F32)
    at = pl.ds(pl.multiple_of(put * 256, 256), 256)
    for h in range(2):
        keys_out[h, pl.ds(0, 128), at] = wide[h * 128:(h + 1) * 128].astype(BF16)
    vals = jnp.dot(ready, vw[...], preferred_element_type=F32)
    for h in range(2):
        vtmp[pl.ds(h, 256, 2), :] = vals[:, h * 128:(h + 1) * 128]
    vals_out[pl.ds(pl.multiple_of(put * 512, 512), 512), :] = vtmp[...].astype(BF16)


def kernel(lat, rot, gain, kup, vup, keys_out, vals_out, rows, gainv, kt, vw,
           latv, stage, rotv, rz, rx, ry, kraw, vraw, wtmp, vtmp,
           loc_sem, send, d_send, xs_recv, xy_recv, z1_recv, z2_recv, d_recv, r_recv):
    e, c, g = lax.axis_index("ens"), lax.axis_index("ctx"), lax.axis_index("group")
    x, y = c % 4, c // 4
    zh, core = g // 2, g % 2
    partner = g + 1 - 2 * core

    def at_xy(xx, yy):
        return (e, yy * 4 + xx, g)

    def at_group(gg):
        return (e, c, gg)

    def remote(src, dst, send, recv, dev):
        return pltpu.make_async_remote_copy(
            src_ref=src, dst_ref=dst, send_sem=send, recv_sem=recv,
            device_id=dev, device_id_type=MESH)

    def got(block, recv):
        remote(block, block, send, recv, at_group(g)).wait_recv()

    def sent(block, sem):
        remote(block, block, sem, xy_recv.at[0], at_group(g)).wait_send()

    barrier = pltpu.get_barrier_semaphore()
    for i in range(1, 4):
        pl.semaphore_signal(barrier, inc=1, device_id=at_xy((x + i) % 4, y), device_id_type=MESH)
        pl.semaphore_signal(barrier, inc=1, device_id=at_xy(x, (y + i) % 4), device_id_type=MESH)
    for gg in ((g + 2) % 8, (g + 6) % 8, partner):
        pl.semaphore_signal(barrier, inc=1, device_id=at_group(gg), device_id_type=MESH)

    local = [
        pltpu.make_async_copy(rot, rotv, loc_sem.at[0]),
        pltpu.make_async_copy(lat.at[c], rows.at[c, g], loc_sem.at[1]),
        pltpu.make_async_copy(lat, latv, loc_sem.at[2]),
        pltpu.make_async_copy(kup, kraw, loc_sem.at[3]),
        pltpu.make_async_copy(vup, vraw, loc_sem.at[4]),
        pltpu.make_async_copy(gain, gainv, loc_sem.at[5]),
    ]
    for copy in local:
        copy.start()
    local[0].wait()
    rz[pl.ds(zh, 1)] = jnp.concatenate([rotv[0:2], rotv[2:4]], axis=-1).reshape(1, 2, 4, 32, 128)
    local[1].wait()
    local[2].wait()
    pl.semaphore_wait(barrier, 9)

    def along(way):
        return at_group((g + 2 + 4 * way) % 8)

    def z1(t, way):
        block = rows.at[column_of(t, x, y), g]
        return remote(block, block, send, z1_recv.at[t], along(way))

    def z2(t):
        way = t % 2
        block = rows.at[column_of(t, x, y), (g + 6 + 4 * way) % 8]
        return remote(block, block, send, z2_recv.at[t % 8], along(way))

    def push(t, hop):
        block = rows.at[column_of(t, x, y), (g + 2 * hop) % 8]
        return remote(block, block, d_send, d_recv.at[t], at_group(partner))

    def x_direct(i):
        to = (x + 4 - gray(i)) % 4
        return remote(latv.at[y * 4 + to], rows.at[c, g], send, xy_recv.at[i], at_xy(to, y))

    def x_stage(i, j):
        to = (x + 4 - gray(i)) % 4
        last = (y + 4 - gray(j)) % 4
        return remote(latv.at[last * 4 + to], stage.at[j - 1, i - 1], send,
                      xs_recv.at[j - 1], at_xy(to, y))

    def y_on(i, j):
        to = (y + 4 - gray(j)) % 4
        src = latv.at[to * 4 + x] if i == 0 else stage.at[j - 1, i - 1]
        return remote(src, rows.at[y * 4 + (x + gray(i)) % 4, g], send,
                      xy_recv.at[order(i, j) if i * j == 0 else 6 + j], at_xy(x, to))

    def rz1(way):
        return remote(rz.at[zh], rz.at[zh], send, r_recv.at[0], along(way))

    def rz2(way):
        block = rz.at[(zh + 3 + 2 * way) % 4, way]
        return remote(block, block, send, r_recv.at[1], along(way))

    def rx_to(i):
        to = (x + 4 - gray(i)) % 4
        return remote(rz.at[:, :, to], rx.at[x], send, r_recv.at[2], at_xy(to, y))

    def ry_to(j):
        to = (y + 4 - gray(j)) % 4
        return remote(rx.at[:, :, to % 2], ry.at[y, :, :, core], send, r_recv.at[3],
                      at_xy(x, to))

    def rpush(j):
        block = ry.at[(y + gray(j)) % 4, :, :, core]
        return remote(block, block, send, r_recv.at[4], at_group(partner))

    for way in range(2):
        z1(0, way).start()
    for way in range(2):
        rz1(way).start()
    for i in range(1, 4):
        x_direct(i).start()
        y_on(0, i).start()
    push(0, 0).start()
    for j in range(1, 4):
        for i in range(1, 4):
            x_stage(i, j).start()

    def forth(t):
        for way in range(2):
            z1(t, way).start()
        push(t, 0).start()

    @pl.loop(1, 16 + LAG_D)
    def _(t):
        @pl.when((t < 4) | ((t > 6) & (t < 16)))
        def _():
            @pl.when(t < 4)
            def _():
                got(rows.at[column_of(t, x, y), g], xy_recv.at[t])

            for j in range(1, 4):
                @pl.when(t == 4 + 3 * j)
                def _(j=j):
                    got(latv.at[pl.ds(0, 3)], xy_recv.at[6 + j])

            forth(t)

        @pl.when(t == 4)
        def _():
            for u in range(4, 7):
                got(rows.at[column_of(u, x, y), g], xy_recv.at[u])
                forth(u)

        for j in range(1, 4):
            @pl.when(t == 3 + j)
            def _(j=j):
                got(stage.at[j - 1], xs_recv.at[j - 1])
                for i in range(1, 4):
                    y_on(i, j).start()

        @pl.when(t == 7)
        def _():
            for copy in local[3:]:
                copy.wait()
            wtmp[...] = kraw[...].astype(F32)
            for h in range(2):
                kt[pl.ds(h * 128, 128), :] = wtmp[pl.ds(h, 512, 2), :].T.astype(BF16)
            wtmp[...] = vraw[...].astype(F32)
            for h in range(2):
                vw[:, pl.ds(h * 128, 128)] = wtmp[pl.ds(h, 512, 2), :].astype(BF16)

        @pl.when((t >= LAG_B) & (t < 16 + LAG_B))
        def _():
            u = t - LAG_B
            got(rows.at[column_of(u, x, y), pl.ds(0, 2)], z1_recv.at[u])
            z2(u).start()
            push(u, 3).start()
            push(u, 1).start()

        @pl.when(t == ROT_Z)
        def _():
            got(rz.at[pl.ds(0, 2)], r_recv.at[0])
            for way in range(2):
                rz2(way).start()

        @pl.when(t == ROT_X)
        def _():
            got(rz.at[0], r_recv.at[1])
            for i in range(1, 4):
                rx_to(i).start()
            rx[pl.ds(x, 1)] = rz[:, :, pl.ds(x, 1)].reshape(1, 4, 2, 32, 128)

        @pl.when(t == ROT_Y)
        def _():
            got(rx.at[pl.ds(0, 3)], r_recv.at[2])
            for j in range(1, 4):
                ry_to(j).start()
            ry[pl.ds(y, 1), :, :, pl.ds(core, 1)] = rx[:, :, pl.ds(y % 2, 1)].reshape(
                1, 4, 4, 1, 32, 128)

        @pl.when(t == ROT_PUSH)
        def _():
            got(ry.at[pl.ds(0, 3), :, :, 0], r_recv.at[3])
            for j in range(4):
                rpush(j).start()

        @pl.when((t >= LAG_C) & (t < 16 + LAG_C))
        def _():
            u = t - LAG_C
            got(rows.at[column_of(u, x, y), 0], z2_recv.at[u % 8])
            push(u, 2).start()

        @pl.when(t >= LAG_D)
        def _():
            u = t - LAG_D
            k = column_of(u, x, y)
            got(rows.at[k, pl.ds(0, 4)], d_recv.at[u])

            @pl.when(u < 16 - LAST)
            def _():
                expand_chunk(k, k, rows, gainv, kt, vw, keys_out, vals_out, vtmp)

        @pl.when(t == ROT_DONE)
        def _():
            got(ry.at[:, :, :, 0], r_recv.at[4])

        @pl.when((t >= ROT_DONE) & (t < ROT_DONE + 4))
        def _():
            lane = lax.broadcasted_iota(jnp.int32, (64, 128), 1)
            number = lax.broadcasted_iota(jnp.int32, (64, 128), 0)
            pick = (lane == number + y // 2 * 64).astype(F32).astype(BF16)
            n = t - ROT_DONE
            one = ry[pl.ds(n, 1)].reshape(1024, 128)
            turned = lax.dot_general(pick, one, (((1,), (1,)), ((), ())),
                                     preferred_element_type=F32).astype(BF16)
            for h in range(2):
                keys_out[h, pl.ds(128, 64), pl.ds(pl.multiple_of(n * 1024, 1024), 1024)] = turned

    sent(rows.at[pl.ds(0, 14)], send)
    sent(rows.at[pl.ds(0, 8)], d_send)


def store(keys_in, vals_in, rows, gainv, kt, vw, keys_out, vals_out, keys_last, vals_last, vtmp,
          keys_sem, vals_sem):
    c = lax.axis_index("ctx")
    x, y = c % 4, c // 4

    def put(k):
        return pl.ds(pl.multiple_of(k * 256, 256), 256), pl.ds(pl.multiple_of(k * 512, 512), 512)

    @pl.loop(0, 16 - LAST)
    def _(t):
        at, to = put(column_of(t, x, y))
        pltpu.make_async_copy(keys_in.at[:, :, at], keys_out.at[:, :, at], keys_sem).start()
        pltpu.make_async_copy(vals_in.at[to], vals_out.at[to], vals_sem).start()

    for n in range(LAST):
        at, to = put(column_of(16 - LAST + n, x, y))
        turned = pl.ds(128, 64)
        pltpu.make_async_copy(keys_in.at[:, turned, at], keys_out.at[:, turned, at],
                              keys_sem).start()

    @pl.loop(0, LAST)
    def _(n):
        k = column_of(16 - LAST + n, x, y)
        expand_chunk(k, n, rows, gainv, kt, vw, keys_last, vals_last, vtmp)

    for n in range(LAST):
        at, to = put(column_of(16 - LAST + n, x, y))
        here, there = put(n)
        pltpu.make_async_copy(keys_last.at[:, :, here], keys_out.at[:, pl.ds(0, 128), at],
                              keys_sem).start()
        pltpu.make_async_copy(vals_last.at[there], vals_out.at[to], vals_sem).start()
    pltpu.make_async_copy(keys_in, keys_out, keys_sem).wait()
    pltpu.make_async_copy(vals_in, vals_out, vals_sem).wait()


def per_device(latents, rotary_rows, latent_gain, key_up, value_up):
    dma = pltpu.SemaphoreType.DMA
    hbm = pl.BlockSpec(memory_space=pltpu.HBM)
    vmem = pl.BlockSpec(memory_space=pltpu.VMEM)
    outs = (
        jax.ShapeDtypeStruct((2, 192, 4096), BF16),
        jax.ShapeDtypeStruct((8192, 128), BF16),
    )
    parts = pl.pallas_call(
        kernel,
        out_shape=outs + (
            jax.ShapeDtypeStruct((16, 8, 32, 512), BF16),
            jax.ShapeDtypeStruct((1, 512), F32),
            jax.ShapeDtypeStruct((256, 512), BF16),
            jax.ShapeDtypeStruct((512, 256), BF16),
        ),
        in_specs=[hbm] * 5,
        out_specs=[vmem] * 6,
        scratch_shapes=[
            pltpu.VMEM((16, 32, 512), BF16),
            pltpu.VMEM((3, 3, 32, 512), BF16),
            pltpu.VMEM((4, 4, 32, 64), BF16),
            pltpu.VMEM((4, 2, 4, 32, 128), BF16),
            pltpu.VMEM((4, 4, 2, 32, 128), BF16),
            pltpu.VMEM((4, 4, 4, 2, 32, 128), BF16),
            pltpu.VMEM((1024, 128), BF16),
            pltpu.VMEM((1024, 128), BF16),
            pltpu.VMEM((1024, 128), F32),
            pltpu.VMEM((512, 128), F32),
            dma((6,)), dma, dma, dma((3,)), dma((10,)), dma((16,)), dma((8,)), dma((16,)), dma((5,)),
        ],
        compiler_params=pltpu.CompilerParams(
            collective_id=0, has_side_effects=True, vmem_limit_bytes=32 * 1024 * 1024),
        name="expand",
    )(*(pltpu.with_memory_space_constraint(a, pltpu.HBM) for a in (
        latents, rotary_rows.reshape(4, 4, 32, 64), latent_gain.reshape(1, 512),
        key_up.reshape(1024, 128), value_up.reshape(1024, 128))))
    keys, vals = pl.pallas_call(
        store,
        out_shape=outs,
        in_specs=[vmem] * 6,
        out_specs=[hbm] * 2,
        scratch_shapes=[
            pltpu.VMEM((2, 128, LAST * 256), BF16),
            pltpu.VMEM((LAST * 512, 128), BF16),
            pltpu.VMEM((512, 128), F32),
            dma, dma,
        ],
        compiler_params=pltpu.CompilerParams(vmem_limit_bytes=32 * 1024 * 1024),
        name="store",
    )(*parts)
    return keys.reshape(1, 2, 192, 4096), vals.reshape(1, 4096, 2, 128)


def solution(mesh):
    in_specs = (
        P("ens", ("ctx", "group"), None),
        P("ens", ("ctx", "group"), None),
        P(),
        P("ens", "group", None),
        P("ens", "group", None),
    )
    out_specs = (P(("ens", "ctx"), "group", None, None), P(("ens", "ctx"), None, "group", None))
    return jax.shard_map(
        per_device, mesh=mesh, in_specs=in_specs, out_specs=out_specs, check_vma=False
    )
```

```python
import jax
import jax.numpy as jnp
from jax import lax
from jax.experimental import pallas as pl
from jax.experimental.pallas import tpu as pltpu
from jax.sharding import PartitionSpec as P

MESH = pl.DeviceIdType.MESH
F32 = jnp.float32
BF16 = jnp.bfloat16
LAG_B, LAG_C, LAG_D = 4, 8, 9
LAST = 2
ROT_Z, ROT_X, ROT_Y, ROT_PUSH, ROT_DONE = 4, 8, 11, 15, 17


def gray(i):
    return i + i // 2 - 2 * (i // 3)


def column_of(t, x, y):
    far, both = (t + 12) // 16, (t + 9) // 16
    i = (1 - far) * t + both * (1 + (t + 2) % 3)
    j = far * (1 - both) * (t - 3) + both * ((t + 2) // 3 - 2)
    return ((y + gray(j)) % 4) * 4 + (x + gray(i)) % 4


def order(i, j):
    return i if j == 0 else 3 + j if i == 0 else 3 + 3 * j + i


def expand_chunk(k, put, rows, gainv, kt, vw, keys_out, vals_out, vtmp):
    one = rows[pl.ds(k, 1)].reshape(256, 512).astype(F32)
    mean = jnp.mean(one * one, axis=-1, keepdims=True)
    ready = (one * lax.rsqrt(mean + 1e-06) * gainv[...]).astype(BF16)
    wide = lax.dot_general(kt[...], ready, (((1,), (1,)), ((), ())),
                           preferred_element_type=F32)
    at = pl.ds(pl.multiple_of(put * 256, 256), 256)
    for h in range(2):
        keys_out[h, pl.ds(0, 128), at] = wide[h * 128:(h + 1) * 128].astype(BF16)
    vals = jnp.dot(ready, vw[...], preferred_element_type=F32)
    for h in range(2):
        vtmp[pl.ds(h, 256, 2), :] = vals[:, h * 128:(h + 1) * 128]
    vals_out[pl.ds(pl.multiple_of(put * 512, 512), 512), :] = vtmp[...].astype(BF16)


def kernel(lat, rot, gain, kup, vup, keys_out, vals_out, rows, gainv, kt, vw,
           latv, stage, rotv, rz, rx, ry, kraw, vraw, wtmp, vtmp,
           loc_sem, send, d_send, xs_recv, xy_recv, z1_recv, z2_recv, d_recv, r_recv):
    e, c, g = lax.axis_index("ens"), lax.axis_index("ctx"), lax.axis_index("group")
    x, y = c % 4, c // 4
    zh, core = g // 2, g % 2
    partner = g + 1 - 2 * core

    def at_xy(xx, yy):
        return (e, yy * 4 + xx, g)

    def at_group(gg):
        return (e, c, gg)

    def remote(src, dst, send, recv, dev):
        return pltpu.make_async_remote_copy(
            src_ref=src, dst_ref=dst, send_sem=send, recv_sem=recv,
            device_id=dev, device_id_type=MESH)

    def got(block, recv):
        remote(block, block, send, recv, at_group(g)).wait_recv()

    def sent(block, sem):
        remote(block, block, sem, xy_recv.at[0], at_group(g)).wait_send()

    barrier = pltpu.get_barrier_semaphore()
    for i in range(1, 4):
        pl.semaphore_signal(barrier, inc=1, device_id=at_xy((x + i) % 4, y), device_id_type=MESH)
        pl.semaphore_signal(barrier, inc=1, device_id=at_xy(x, (y + i) % 4), device_id_type=MESH)
    for gg in ((g + 2) % 8, (g + 6) % 8, partner):
        pl.semaphore_signal(barrier, inc=1, device_id=at_group(gg), device_id_type=MESH)

    local = [
        pltpu.make_async_copy(rot, rotv, loc_sem.at[0]),
        pltpu.make_async_copy(lat.at[c], rows.at[c, g], loc_sem.at[1]),
        pltpu.make_async_copy(lat, latv, loc_sem.at[2]),
        pltpu.make_async_copy(kup, kraw, loc_sem.at[3]),
        pltpu.make_async_copy(vup, vraw, loc_sem.at[4]),
        pltpu.make_async_copy(gain, gainv, loc_sem.at[5]),
    ]
    for copy in local:
        copy.start()
    local[0].wait()
    rz[pl.ds(zh, 1)] = jnp.concatenate([rotv[0:2], rotv[2:4]], axis=-1).reshape(1, 2, 4, 32, 128)
    local[1].wait()
    local[2].wait()
    pl.semaphore_wait(barrier, 9)

    def along(way):
        return at_group((g + 2 + 4 * way) % 8)

    def z1(t, way):
        block = rows.at[column_of(t, x, y), g]
        return remote(block, block, send, z1_recv.at[t], along(way))

    def z2(t):
        way = t % 2
        block = rows.at[column_of(t, x, y), (g + 6 + 4 * way) % 8]
        return remote(block, block, send, z2_recv.at[t % 8], along(way))

    def push(t, hop):
        block = rows.at[column_of(t, x, y), (g + 2 * hop) % 8]
        return remote(block, block, d_send, d_recv.at[t], at_group(partner))

    def x_direct(i):
        to = (x + 4 - gray(i)) % 4
        return remote(latv.at[y * 4 + to], rows.at[c, g], send, xy_recv.at[i], at_xy(to, y))

    def x_stage(i, j):
        to = (x + 4 - gray(i)) % 4
        last = (y + 4 - gray(j)) % 4
        return remote(latv.at[last * 4 + to], stage.at[j - 1, i - 1], send,
                      xs_recv.at[j - 1], at_xy(to, y))

    def y_on(i, j):
        to = (y + 4 - gray(j)) % 4
        src = latv.at[to * 4 + x] if i == 0 else stage.at[j - 1, i - 1]
        return remote(src, rows.at[y * 4 + (x + gray(i)) % 4, g], send,
                      xy_recv.at[order(i, j) if i * j == 0 else 6 + j], at_xy(x, to))

    def rz1(way):
        return remote(rz.at[zh], rz.at[zh], send, r_recv.at[0], along(way))

    def rz2(way):
        block = rz.at[(zh + 3 + 2 * way) % 4, way]
        return remote(block, block, send, r_recv.at[1], along(way))

    def rx_to(i):
        to = (x + 4 - gray(i)) % 4
        return remote(rz.at[:, :, to], rx.at[x], send, r_recv.at[2], at_xy(to, y))

    def ry_to(j):
        to = (y + 4 - gray(j)) % 4
        return remote(rx.at[:, :, to % 2], ry.at[y, :, :, core], send, r_recv.at[3],
                      at_xy(x, to))

    def rpush(j):
        block = ry.at[(y + gray(j)) % 4, :, :, core]
        return remote(block, block, send, r_recv.at[4], at_group(partner))

    for way in range(2):
        z1(0, way).start()
    for way in range(2):
        rz1(way).start()
    for i in range(1, 4):
        x_direct(i).start()
        y_on(0, i).start()
    push(0, 0).start()
    for j in range(1, 4):
        for i in range(1, 4):
            x_stage(i, j).start()

    def forth(t):
        for way in range(2):
            z1(t, way).start()
        push(t, 0).start()

    @pl.loop(1, 16 + LAG_D)
    def _(t):
        @pl.when((t >= LAG_C) & (t < 16 + LAG_C))
        def _():
            u = t - LAG_C
            got(rows.at[column_of(u, x, y), 0], z2_recv.at[u % 8])
            push(u, 2).start()

        @pl.when((t < 4) | ((t > 6) & (t < 16)))
        def _():
            @pl.when(t < 4)
            def _():
                got(rows.at[column_of(t, x, y), g], xy_recv.at[t])

            for j in range(1, 4):
                @pl.when(t == 4 + 3 * j)
                def _(j=j):
                    got(latv.at[pl.ds(0, 3)], xy_recv.at[6 + j])

            forth(t)

        @pl.when(t == 4)
        def _():
            for u in range(4, 7):
                got(rows.at[column_of(u, x, y), g], xy_recv.at[u])
                forth(u)

        for j in range(1, 4):
            @pl.when(t == 3 + j)
            def _(j=j):
                got(stage.at[j - 1], xs_recv.at[j - 1])
                for i in range(1, 4):
                    y_on(i, j).start()

        @pl.when(t == 7)
        def _():
            for copy in local[3:]:
                copy.wait()
            wtmp[...] = kraw[...].astype(F32)
            for h in range(2):
                kt[pl.ds(h * 128, 128), :] = wtmp[pl.ds(h, 512, 2), :].T.astype(BF16)
            wtmp[...] = vraw[...].astype(F32)
            for h in range(2):
                vw[:, pl.ds(h * 128, 128)] = wtmp[pl.ds(h, 512, 2), :].astype(BF16)

        @pl.when(t >= LAG_D)
        def _():
            u = t - LAG_D
            k = column_of(u, x, y)
            got(rows.at[k, pl.ds(0, 4)], d_recv.at[u])

            @pl.when(u < 16 - LAST)
            def _():
                expand_chunk(k, k, rows, gainv, kt, vw, keys_out, vals_out, vtmp)

        @pl.when((t >= LAG_B) & (t < 16 + LAG_B))
        def _():
            u = t - LAG_B
            got(rows.at[column_of(u, x, y), pl.ds(0, 2)], z1_recv.at[u])
            z2(u).start()
            push(u, 3).start()
            push(u, 1).start()

        @pl.when(t == ROT_Z)
        def _():
            got(rz.at[pl.ds(0, 2)], r_recv.at[0])
            for way in range(2):
                rz2(way).start()

        @pl.when(t == ROT_X)
        def _():
            got(rz.at[0], r_recv.at[1])
            for i in range(1, 4):
                rx_to(i).start()
            rx[pl.ds(x, 1)] = rz[:, :, pl.ds(x, 1)].reshape(1, 4, 2, 32, 128)

        @pl.when(t == ROT_Y)
        def _():
            got(rx.at[pl.ds(0, 3)], r_recv.at[2])
            for j in range(1, 4):
                ry_to(j).start()
            ry[pl.ds(y, 1), :, :, pl.ds(core, 1)] = rx[:, :, pl.ds(y % 2, 1)].reshape(
                1, 4, 4, 1, 32, 128)

        @pl.when(t == ROT_PUSH)
        def _():
            got(ry.at[pl.ds(0, 3), :, :, 0], r_recv.at[3])
            for j in range(4):
                rpush(j).start()

        @pl.when(t == ROT_DONE)
        def _():
            got(ry.at[:, :, :, 0], r_recv.at[4])

        @pl.when((t >= ROT_DONE) & (t < ROT_DONE + 4))
        def _():
            lane = lax.broadcasted_iota(jnp.int32, (64, 128), 1)
            number = lax.broadcasted_iota(jnp.int32, (64, 128), 0)
            pick = (lane == number + y // 2 * 64).astype(F32).astype(BF16)
            n = t - ROT_DONE
            one = ry[pl.ds(n, 1)].reshape(1024, 128)
            turned = lax.dot_general(pick, one, (((1,), (1,)), ((), ())),
                                     preferred_element_type=F32).astype(BF16)
            for h in range(2):
                keys_out[h, pl.ds(128, 64), pl.ds(pl.multiple_of(n * 1024, 1024), 1024)] = turned

    sent(rows.at[pl.ds(0, 14)], send)
    sent(rows.at[pl.ds(0, 8)], d_send)


def store(keys_in, vals_in, rows, gainv, kt, vw, keys_out, vals_out, keys_last, vals_last, vtmp,
          keys_sem, vals_sem):
    c = lax.axis_index("ctx")
    x, y = c % 4, c // 4

    def put(k):
        return pl.ds(pl.multiple_of(k * 256, 256), 256), pl.ds(pl.multiple_of(k * 512, 512), 512)

    @pl.loop(0, 16 - LAST)
    def _(t):
        at, to = put(column_of(t, x, y))
        pltpu.make_async_copy(keys_in.at[:, :, at], keys_out.at[:, :, at], keys_sem).start()
        pltpu.make_async_copy(vals_in.at[to], vals_out.at[to], vals_sem).start()

    for n in range(LAST):
        at, to = put(column_of(16 - LAST + n, x, y))
        turned = pl.ds(128, 64)
        pltpu.make_async_copy(keys_in.at[:, turned, at], keys_out.at[:, turned, at],
                              keys_sem).start()

    @pl.loop(0, LAST)
    def _(n):
        k = column_of(16 - LAST + n, x, y)
        expand_chunk(k, n, rows, gainv, kt, vw, keys_last, vals_last, vtmp)

    for n in range(LAST):
        at, to = put(column_of(16 - LAST + n, x, y))
        here, there = put(n)
        pltpu.make_async_copy(keys_last.at[:, :, here], keys_out.at[:, pl.ds(0, 128), at],
                              keys_sem).start()
        pltpu.make_async_copy(vals_last.at[there], vals_out.at[to], vals_sem).start()
    pltpu.make_async_copy(keys_in, keys_out, keys_sem).wait()
    pltpu.make_async_copy(vals_in, vals_out, vals_sem).wait()


def per_device(latents, rotary_rows, latent_gain, key_up, value_up):
    dma = pltpu.SemaphoreType.DMA
    hbm = pl.BlockSpec(memory_space=pltpu.HBM)
    vmem = pl.BlockSpec(memory_space=pltpu.VMEM)
    outs = (
        jax.ShapeDtypeStruct((2, 192, 4096), BF16),
        jax.ShapeDtypeStruct((8192, 128), BF16),
    )
    parts = pl.pallas_call(
        kernel,
        out_shape=outs + (
            jax.ShapeDtypeStruct((16, 8, 32, 512), BF16),
            jax.ShapeDtypeStruct((1, 512), F32),
            jax.ShapeDtypeStruct((256, 512), BF16),
            jax.ShapeDtypeStruct((512, 256), BF16),
        ),
        in_specs=[hbm] * 5,
        out_specs=[vmem] * 6,
        scratch_shapes=[
            pltpu.VMEM((16, 32, 512), BF16),
            pltpu.VMEM((3, 3, 32, 512), BF16),
            pltpu.VMEM((4, 4, 32, 64), BF16),
            pltpu.VMEM((4, 2, 4, 32, 128), BF16),
            pltpu.VMEM((4, 4, 2, 32, 128), BF16),
            pltpu.VMEM((4, 4, 4, 2, 32, 128), BF16),
            pltpu.VMEM((1024, 128), BF16),
            pltpu.VMEM((1024, 128), BF16),
            pltpu.VMEM((1024, 128), F32),
            pltpu.VMEM((512, 128), F32),
            dma((6,)), dma, dma, dma((3,)), dma((10,)), dma((16,)), dma((8,)), dma((16,)), dma((5,)),
        ],
        compiler_params=pltpu.CompilerParams(
            collective_id=0, has_side_effects=True, vmem_limit_bytes=32 * 1024 * 1024),
        name="expand",
    )(*(pltpu.with_memory_space_constraint(a, pltpu.HBM) for a in (
        latents, rotary_rows.reshape(4, 4, 32, 64), latent_gain.reshape(1, 512),
        key_up.reshape(1024, 128), value_up.reshape(1024, 128))))
    keys, vals = pl.pallas_call(
        store,
        out_shape=outs,
        in_specs=[vmem] * 6,
        out_specs=[hbm] * 2,
        scratch_shapes=[
            pltpu.VMEM((2, 128, LAST * 256), BF16),
            pltpu.VMEM((LAST * 512, 128), BF16),
            pltpu.VMEM((512, 128), F32),
            dma, dma,
        ],
        compiler_params=pltpu.CompilerParams(vmem_limit_bytes=32 * 1024 * 1024),
        name="store",
    )(*parts)
    return keys.reshape(1, 2, 192, 4096), vals.reshape(1, 4096, 2, 128)


def solution(mesh):
    in_specs = (
        P("ens", ("ctx", "group"), None),
        P("ens", ("ctx", "group"), None),
        P(),
        P("ens", "group", None),
        P("ens", "group", None),
    )
    out_specs = (P(("ens", "ctx"), "group", None, None), P(("ens", "ctx"), None, "group", None))
    return jax.shard_map(
        per_device, mesh=mesh, in_specs=in_specs, out_specs=out_specs, check_vma=False
    )
```
